32 devices in a mesh: ia: 4 (over y, x), ja: 4 (over z), col: 2 (over core).
Axes of the slice: x: 2, y: 2, z: 4, core: 2. Of those that a mesh axis runs over, the one named last changes fastest.
Arguments:
- pair_rep: bfloat16 [512, 512, 128], P('ia', 'ja'), may hold values from -6 to 6
- norm_gain: float32 [128], replicated, may hold values from 0.1 to 1.9
- weights: bfloat16 [4, 128, 128], P(None, None, 'col'), may hold values from -0.5 to 0.5
- residue_mask: int32 [512], replicated, may hold values 0 or 1
- product_grad: bfloat16 [512, 128, 512], P('ia', 'col', 'ja'), may hold values from -1 to 1
Outputs:
- pair_grad: bfloat16 [512, 512, 128], P('ia', 'ja')
- weight_grads: float32 [4, 128, 128], P(None, None, 'col')
The draws below stay inside these ranges and needn't reach their ends.
All inputs are finite; a program needn't handle non-finite values.
Results may differ from the reference program's by a relative error of at most 0.0067.
Values may be sent and summed in bfloat16 or wider, within the bound.
A program may use at most 128 MiB of HBM per device.

```python
import jax
import jax.numpy as jnp
from jax import lax

C = 128
HID = 128
N = 512


def draw_product_grad(key, part):
    gaussian = jax.random.normal(jax.random.fold_in(key, 11), (N, HID, N), jnp.float32)
    drawn = 0.0625 * gaussian
    return jnp.clip(drawn, -1.0, 1.0).astype(jnp.bfloat16)


def set_ends(result, own_key, least, largest):
    longest = result.shape.index(max(result.shape))
    spots = []
    for shift in (0, 1):
        where = [jax.random.randint(jax.random.fold_in(own_key, axis), (), 0, length) for axis, length in enumerate(result.shape)]
        where[longest] = (where[longest] + shift) % result.shape[longest]
        spots.append(tuple(where))
    return result.at[spots[0]].set(least).at[spots[1]].set(largest)


def levels(rng, extent, shards, least, largest):
    level, own = 1.0, jax.random.fold_in(rng, 6)
    for dim, blocks in shards:
        steps = jnp.exp(jax.random.uniform(jax.random.fold_in(own, dim), (blocks,), jnp.float32, least / len(shards), largest / len(shards)))
        level = level * jnp.repeat(steps, extent[dim] // blocks).reshape([-1 if axis == dim else 1 for axis in range(len(extent))])
    return level


def noise(stream_key, dims, width, reach, shards=(), held_as=jnp.bfloat16):
    level = levels(stream_key, dims, shards, -0.22, 0.18) if shards else 1.0
    entries = jax.random.normal(stream_key, dims, jnp.float32) * width * level
    return jnp.minimum(jnp.maximum(entries, -reach), reach).astype(held_as)


def setup_inputs(seed: int = 0) -> dict:
    seeds = jax.random.split(jax.random.key(seed), 6)
    pair_rep = noise(seeds[0], (N, N, C), 1.0, 6.0, ((0, 4), (1, 4)))
    norm_gain = jnp.clip(1.0 + 0.18 * jax.random.normal(seeds[1], (C,), jnp.float32), 0.1, 1.9)
    weights = noise(seeds[2], (4, C, HID), C ** -0.5, 0.5, ((2, 2),))
    residue_mask = set_ends((jax.random.randint(seeds[3], (N,), 0, 8) < 7).astype(jnp.int32), jax.random.fold_in(seeds[3], 1), 0, 1)
    product_grad = draw_product_grad(jax.random.fold_in(seeds[5], 71), 0)
    return {"pair_rep": pair_rep, "norm_gain": norm_gain, "weights": weights, "residue_mask": residue_mask, "product_grad": product_grad}


CLIP_LIMIT = 64.0

def gate_terms(incoming, linear, gate_pre, pair_valid):
    sigmoid_gate = jax.nn.sigmoid(gate_pre)
    through = incoming * pair_valid
    return (through * sigmoid_gate, through * linear * sigmoid_gate * (1.0 - sigmoid_gate))

def reference(pair_rep, norm_gain, weights, residue_mask, product_grad):
    floats = pair_rep.astype(jnp.float32)
    centred = floats - lax.optimization_barrier(jnp.mean(floats, axis=-1, keepdims=True))
    inv_std = lax.rsqrt(lax.optimization_barrier(jnp.mean(centred * centred, axis=-1, keepdims=True)) + 1e-05)
    unit_rows = centred * inv_std
    normed = (unit_rows * norm_gain).astype(jnp.bfloat16)
    validity = residue_mask.astype(jnp.float32)
    pair_valid = validity[:, None, None] * validity[None, None, :]
    normed_wide = normed.astype(jnp.float32)
    weights_wide = weights.astype(jnp.float32)
    projected = [jnp.einsum('ikd,dc->ick', normed_wide, weights_wide[which]) for which in range(4)]
    left_side = (pair_valid * jax.nn.sigmoid(projected[1]) * projected[0]).astype(jnp.bfloat16)
    right_side = (pair_valid * jax.nn.sigmoid(projected[3]) * projected[2]).astype(jnp.bfloat16)
    grad_wide = product_grad.astype(jnp.float32)
    grad_left = jnp.einsum('icj,jck->ick', grad_wide, right_side.astype(jnp.float32))
    grad_right = jnp.einsum('icj,ick->jck', grad_wide, left_side.astype(jnp.float32))
    lin_a, gate_a = gate_terms(grad_left, projected[0], projected[1], pair_valid)
    lin_b, gate_b = gate_terms(grad_right, projected[2], projected[3], pair_valid)
    raw_list = []
    normed_grad = jnp.zeros(floats.shape, jnp.float32)
    for which, term in enumerate((lin_a, gate_a, lin_b, gate_b)):
        rounded = lax.optimization_barrier(term.astype(jnp.bfloat16)).astype(jnp.float32)
        raw_list.append(jnp.einsum('ikd,ick->dc', normed_wide, rounded))
        normed_grad = normed_grad + jnp.einsum('ick,dc->ikd', rounded, weights_wide[which])
    scaled = normed_grad * norm_gain
    pair_grad = inv_std * (scaled - lax.optimization_barrier(jnp.mean(scaled, axis=-1, keepdims=True)) - unit_rows * lax.optimization_barrier(jnp.mean(scaled * unit_rows, axis=-1, keepdims=True)))
    raw = jnp.stack(raw_list)
    squares = jnp.sum(raw * raw)
    factor = jnp.minimum(1.0, CLIP_LIMIT * lax.rsqrt(squares + 1e-06))
    return (pair_grad.astype(jnp.bfloat16), raw * factor)
```

```python
import math

import jax
import jax.numpy as jnp
from jax import lax
from jax.sharding import PartitionSpec as P

CLIP_LIMIT = 64.0
MAX_CHUNKS = 4


def partner(index, step, count):
    if count & (count - 1) == 0:
        return index ^ step
    return (step - index + count) % count


def exchange(value, axis, step, count):
    return lax.ppermute(value, axis, [(a, partner(a, step, count)) for a in range(count)])


def on_device(rows_n, cols_n, halves_n, pair_rep, norm_gain, weights, residue_mask, product_grad):
    row_count, col_count, depth = pair_rep.shape
    channels = product_grad.shape[1]
    block = channels // rows_n
    chunks = math.gcd(block, MAX_CHUNKS)
    part = block // chunks
    me = lax.axis_index("ia")
    others = [partner(me, step, rows_n) for step in range(rows_n)]

    by_channel = product_grad.transpose(1, 0, 2).reshape(rows_n, chunks, part, row_count, col_count)
    panels = []
    for q in range(chunks):
        pieces = []
        for step in range(rows_n):
            mine = lax.dynamic_index_in_dim(by_channel[:, q], others[step], 0, keepdims=False)
            pieces.append(mine if step == 0 else exchange(mine, "ia", step, rows_n))
        local = jnp.stack(pieces, axis=1).reshape(part, rows_n * row_count, col_count)
        panels.append(lax.all_gather(local, "ja", axis=2, tiled=True))

    by_block = weights.reshape(4, depth, rows_n, chunks, part)
    ordered = jnp.stack(
        [lax.dynamic_index_in_dim(by_block, other, 2, keepdims=False) for other in others], axis=3
    ).reshape(4, depth, channels)

    validity = residue_mask.astype(jnp.float32)
    row_valid = lax.dynamic_slice_in_dim(validity, me * row_count, row_count)
    col_valid = lax.dynamic_slice_in_dim(
        validity, lax.axis_index("ja") * col_count, col_count
    )
    pair_valid = row_valid[:, None] * col_valid[None, :]
    floats = pair_rep.astype(jnp.float32)
    centred = floats - jnp.mean(floats, axis=-1, keepdims=True)
    inv_std = lax.rsqrt(jnp.mean(centred * centred, axis=-1, keepdims=True) + 1e-05)
    unit_rows = centred * inv_std
    normed = (unit_rows * norm_gain).astype(jnp.bfloat16)
    projected = jnp.einsum(
        "wdc,ikd->wcik", ordered, normed, preferred_element_type=jnp.float32
    )
    left = (pair_valid * jax.nn.sigmoid(projected[1]) * projected[0]).astype(jnp.bfloat16)
    right = (pair_valid * jax.nn.sigmoid(projected[3]) * projected[2]).astype(jnp.bfloat16)
    split = (chunks, rows_n, part, row_count, col_count)
    both = jnp.stack([left.reshape(split), right.reshape(split)])
    left_pieces = []
    right_full = jnp.zeros((chunks, part, rows_n, row_count, col_count), jnp.bfloat16)
    for step in range(rows_n):
        mine = both[:, :, step]
        came = mine if step == 0 else exchange(mine, "ia", step, rows_n)
        left_pieces.append(came[0])
        right_full = lax.dynamic_update_index_in_dim(right_full, came[1], others[step], 2)
    left_full = jnp.stack(left_pieces, axis=2)
    rows_all = rows_n * row_count
    left_full = left_full.reshape(chunks, part, rows_all, col_count)
    right_full = right_full.reshape(chunks, part, rows_all, col_count)

    terms = []
    chunk_channels = rows_n * part
    for q in range(chunks):
        grad_left = jnp.einsum(
            "cij,cjk->cik", panels[q], right_full[q], preferred_element_type=jnp.bfloat16
        ).reshape(part, rows_n, row_count, col_count)
        grad_right = jnp.einsum(
            "cij,cik->cjk", panels[q], left_full[q], preferred_element_type=jnp.bfloat16
        ).reshape(part, rows_n, row_count, col_count)
        back_left, back_right = [], []
        for step in range(rows_n):
            mine_left = grad_left[:, step]
            mine_right = lax.dynamic_index_in_dim(grad_right, others[step], 1, keepdims=False)
            if step:
                mine_left = exchange(mine_left, "ia", step, rows_n)
                mine_right = exchange(mine_right, "ia", step, rows_n)
            back_left.append(mine_left)
            back_right.append(mine_right)
        where = slice(q * chunk_channels, (q + 1) * chunk_channels)
        own = projected[:, where]
        for pieces, linear, gate_pre in ((back_left, own[0], own[1]), (back_right, own[2], own[3])):
            through = jnp.concatenate(pieces, axis=0).astype(jnp.float32) * pair_valid
            gate = jax.nn.sigmoid(gate_pre)
            terms.append(
                jnp.stack([through * gate, through * linear * gate * (1.0 - gate)]).astype(jnp.bfloat16)
            )
    proj_grads = jnp.concatenate(
        [jnp.concatenate(terms[side::2], axis=1) for side in (0, 1)], axis=0
    )
    grad_part = jnp.einsum("wcik,ikd->wcd", proj_grads, normed, preferred_element_type=jnp.float32)
    grad_part = grad_part.reshape(4, chunks, rows_n, part, depth)
    raw = jnp.zeros((4, rows_n, chunks, part, depth), jnp.float32)
    for step in range(rows_n):
        raw = lax.dynamic_update_index_in_dim(raw, grad_part[:, :, step], others[step], 1)
    raw = raw.reshape(4, channels, depth).transpose(0, 2, 1)
    summed = lax.psum(raw, ("ia", "ja"))
    squares = lax.psum(jnp.sum(summed * summed), "col")
    factor = jnp.minimum(1.0, CLIP_LIMIT * lax.rsqrt(squares + 1e-06))
    weight_grads = summed * factor

    if halves_n == 2:
        input_part = jnp.einsum(
            "wcik,wdc->ikd", proj_grads, ordered, preferred_element_type=jnp.bfloat16
        )
        input_part = lax.optimization_barrier(input_part)
        came = exchange(input_part, "col", 1, halves_n)
        normed_grad = input_part.astype(jnp.float32) + came.astype(jnp.float32)
    else:
        normed_grad = lax.psum(
            jnp.einsum("wcik,wdc->ikd", proj_grads, ordered, preferred_element_type=jnp.float32),
            "col",
        )
    scaled = normed_grad * norm_gain
    pair_grad = inv_std * (
        scaled
        - jnp.mean(scaled, axis=-1, keepdims=True)
        - unit_rows * jnp.mean(scaled * unit_rows, axis=-1, keepdims=True)
    )
    return (pair_grad.astype(jnp.bfloat16), weight_grads)


def solution(mesh):
    sizes = mesh.shape["ia"], mesh.shape["ja"], mesh.shape["col"]
    placed = (P("ia", "ja", None), P(), P(None, None, "col"), P(), P("ia", "col", "ja"))

    def step(*args):
        return on_device(*sizes, *args)

    return jax.shard_map(
        step,
        mesh=mesh,
        in_specs=placed,
        out_specs=(P("ia", "ja", None), P(None, None, "col")),
        check_vma=False,
    )
```

```python
import math

import jax
import jax.numpy as jnp
from jax import lax
from jax.sharding import PartitionSpec as P

CLIP_LIMIT = 64.0
MAX_CHUNKS = 2


def partner(index, step, count):
    if count & (count - 1) == 0:
        return index ^ step
    return (step - index + count) % count


def exchange(value, axis, step, count):
    return lax.ppermute(value, axis, [(a, partner(a, step, count)) for a in range(count)])


def on_device(rows_n, cols_n, halves_n, pair_rep, norm_gain, weights, residue_mask, product_grad):
    row_count, col_count, depth = pair_rep.shape
    channels = product_grad.shape[1]
    block = channels // rows_n
    chunks = math.gcd(block, MAX_CHUNKS)
    part = block // chunks
    me = lax.axis_index("ia")
    others = [partner(me, step, rows_n) for step in range(rows_n)]

    by_channel = product_grad.transpose(1, 0, 2).reshape(rows_n, chunks, part, row_count, col_count)
    panels = []
    for q in range(chunks):
        pieces = []
        for step in range(rows_n):
            mine = lax.dynamic_index_in_dim(by_channel[:, q], others[step], 0, keepdims=False)
            pieces.append(mine if step == 0 else exchange(mine, "ia", step, rows_n))
        local = jnp.stack(pieces, axis=1).reshape(part, rows_n * row_count, col_count)
        panels.append(lax.all_gather(local, "ja", axis=2, tiled=True))

    by_block = weights.reshape(4, depth, rows_n, chunks, part)
    ordered = jnp.stack(
        [lax.dynamic_index_in_dim(by_block, other, 2, keepdims=False) for other in others], axis=3
    ).reshape(4, depth, channels)

    validity = residue_mask.astype(jnp.float32)
    row_valid = lax.dynamic_slice_in_dim(validity, me * row_count, row_count)
    col_valid = lax.dynamic_slice_in_dim(
        validity, lax.axis_index("ja") * col_count, col_count
    )
    pair_valid = row_valid[:, None] * col_valid[None, :]
    floats = pair_rep.astype(jnp.float32)
    centred = floats - jnp.mean(floats, axis=-1, keepdims=True)
    inv_std = lax.rsqrt(jnp.mean(centred * centred, axis=-1, keepdims=True) + 1e-05)
    unit_rows = centred * inv_std
    normed = (unit_rows * norm_gain).astype(jnp.bfloat16)
    projected = jnp.einsum(
        "wdc,ikd->wcik", ordered, normed, preferred_element_type=jnp.float32
    )
    left = (pair_valid * jax.nn.sigmoid(projected[1]) * projected[0]).astype(jnp.bfloat16)
    right = (pair_valid * jax.nn.sigmoid(projected[3]) * projected[2]).astype(jnp.bfloat16)
    split = (chunks, rows_n, part, row_count, col_count)
    both = jnp.stack([left.reshape(split), right.reshape(split)])
    left_pieces = []
    right_full = jnp.zeros((chunks, part, rows_n, row_count, col_count), jnp.bfloat16)
    for step in range(rows_n):
        mine = both[:, :, step]
        came = mine if step == 0 else exchange(mine, "ia", step, rows_n)
        left_pieces.append(came[0])
        right_full = lax.dynamic_update_index_in_dim(right_full, came[1], others[step], 2)
    left_full = jnp.stack(left_pieces, axis=2)
    rows_all = rows_n * row_count
    left_full = left_full.reshape(chunks, part, rows_all, col_count)
    right_full = right_full.reshape(chunks, part, rows_all, col_count)

    terms = []
    chunk_channels = rows_n * part
    for q in range(chunks):
        grad_left = jnp.einsum(
            "cij,cjk->cik", panels[q], right_full[q], preferred_element_type=jnp.bfloat16
        ).reshape(part, rows_n, row_count, col_count)
        grad_right = jnp.einsum(
            "cij,cik->cjk", panels[q], left_full[q], preferred_element_type=jnp.bfloat16
        ).reshape(part, rows_n, row_count, col_count)
        back_left, back_right = [], []
        for step in range(rows_n):
            mine_right = lax.dynamic_index_in_dim(grad_right, others[step], 1, keepdims=False)
            pair = jnp.stack([grad_left[:, step], mine_right])
            if step:
                pair = exchange(pair, "ia", step, rows_n)
            back_left.append(pair[0])
            back_right.append(pair[1])
        where = slice(q * chunk_channels, (q + 1) * chunk_channels)
        own = projected[:, where]
        for pieces, linear, gate_pre in ((back_left, own[0], own[1]), (back_right, own[2], own[3])):
            through = jnp.concatenate(pieces, axis=0).astype(jnp.float32) * pair_valid
            gate = jax.nn.sigmoid(gate_pre)
            terms.append(
                jnp.stack([through * gate, through * linear * gate * (1.0 - gate)]).astype(jnp.bfloat16)
            )
    proj_grads = jnp.concatenate(
        [jnp.concatenate(terms[side::2], axis=1) for side in (0, 1)], axis=0
    )
    grad_part = jnp.einsum("wcik,ikd->wcd", proj_grads, normed, preferred_element_type=jnp.float32)
    grad_part = grad_part.reshape(4, chunks, rows_n, part, depth)
    raw = jnp.zeros((4, rows_n, chunks, part, depth), jnp.float32)
    for step in range(rows_n):
        raw = lax.dynamic_update_index_in_dim(raw, grad_part[:, :, step], others[step], 1)
    raw = raw.reshape(4, channels, depth).transpose(0, 2, 1)
    summed = raw
    for axis, count in (("ia", rows_n), ("ja", cols_n)):
        if count & (count - 1):
            summed = lax.psum(summed, axis)
            continue
        step = 1
        while step < count:
            summed = summed + exchange(summed, axis, step, count)
            step *= 2
    squares = lax.psum(jnp.sum(summed * summed), "col")
    factor = jnp.minimum(1.0, CLIP_LIMIT * lax.rsqrt(squares + 1e-06))
    weight_grads = summed * factor

    if halves_n == 2:
        input_part = jnp.einsum(
            "wcik,wdc->ikd", proj_grads, ordered, preferred_element_type=jnp.bfloat16
        )
        input_part = lax.optimization_barrier(input_part)
        came = exchange(input_part, "col", 1, halves_n)
        normed_grad = input_part.astype(jnp.float32) + came.astype(jnp.float32)
    else:
        normed_grad = lax.psum(
            jnp.einsum("wcik,wdc->ikd", proj_grads, ordered, preferred_element_type=jnp.float32),
            "col",
        )
    scaled = normed_grad * norm_gain
    pair_grad = inv_std * (
        scaled
        - jnp.mean(scaled, axis=-1, keepdims=True)
        - unit_rows * jnp.mean(scaled * unit_rows, axis=-1, keepdims=True)
    )
    return (pair_grad.astype(jnp.bfloat16), weight_grads)


def solution(mesh):
    sizes = mesh.shape["ia"], mesh.shape["ja"], mesh.shape["col"]
    placed = (P("ia", "ja", None), P(), P(None, None, "col"), P(), P("ia", "col", "ja"))

    def step(*args):
        return on_device(*sizes, *args)

    return jax.shard_map(
        step,
        mesh=mesh,
        in_specs=placed,
        out_specs=(P("ia", "ja", None), P(None, None, "col")),
        check_vma=False,
    )
```
